128 devices in a mesh: seg: 64 (over y, z_hi, x, core), freq: 2 (over z_lo).
Axes of the slice: x: 4, y: 4, z: 4 (z_hi: 2, z_lo: 2; z = z_hi * 2 + z_lo), core: 2. Of those that a mesh axis runs over, the one named last changes fastest.
Arguments:
- coarse: float32 [256, 512, 2048], P('seg', None, 'freq'), may hold values from 0.5 to 8
- offsets: int32 [256, 32], replicated, may hold values from -8 to 8, as said below
Outputs:
- fine: float32 [32, 512, 2048], P(None, 'seg', 'freq')
- peaks: float32 [512], P('seg')
The draws below stay inside these ranges and needn't reach their ends.
Inputs may be any that keep to these rules, and one draw needn't show every extreme that they name: `offsets`: every entry lies in -8 to 8, and both ends occur in every draw.
All inputs are finite; a program needn't handle non-finite values.
Results may differ from the reference program's by a relative error of at most 0.0003.
Values sent between devices are 32-bit elements; how exact they have to be, the bound alone decides.
No kernel may reach another device: no remote copies, remote signals or barrier semaphores. Data moves between devices by JAX's collectives and lax.ppermute only.
A program may use at most 128 MiB of HBM per device.

```python
import math
import jax
import jax.numpy as jnp
from jax import lax

SPINDOWNS = 32
HALO = 8
SEGMENTS = 256
SKY_POINTS = 512
BINS = 2048


def draw_offsets(key, part):
    base = jax.random.randint(jax.random.fold_in(key, 11), (SEGMENTS, SPINDOWNS), -HALO, HALO + 1, dtype=jnp.int32)
    first_seg = jax.random.randint(jax.random.fold_in(key, 12), (), 0, SEGMENTS, dtype=jnp.int32)
    step_seg = jax.random.randint(jax.random.fold_in(key, 13), (), 1, SEGMENTS, dtype=jnp.int32)
    second_seg = (first_seg + step_seg) % SEGMENTS
    first_spin = jax.random.randint(jax.random.fold_in(key, 14), (), 0, SPINDOWNS, dtype=jnp.int32)
    second_spin = jax.random.randint(jax.random.fold_in(key, 15), (), 0, SPINDOWNS, dtype=jnp.int32)
    base = base.at[first_seg, first_spin].set(HALO)
    base = base.at[second_seg, second_spin].set(-HALO)
    return base


def shard_levels(stream_key, shape, pieces, smallest, largest):
    gain = 1.0
    for dim, parts in pieces:
        steps = jax.random.uniform(jax.random.fold_in(jax.random.fold_in(stream_key, 6), dim), (parts,), jnp.float32, smallest / len(pieces), largest / len(pieces))
        gain = gain * jnp.repeat(jnp.exp(steps), shape[dim] // parts).reshape((-1,) + (1,) * (len(shape) - 1 - dim))
    return gain


def setup_inputs(seed: int = 0) -> dict:
    streams_of = jax.random.split(jax.random.key(seed), 3)
    coarse = jnp.clip(jnp.exp(math.log(8.0) - 2.7725887 * jax.random.uniform(streams_of[0], (SEGMENTS, SKY_POINTS, BINS), jnp.float32) ** shard_levels(streams_of[0], (SEGMENTS, SKY_POINTS, BINS), ((0, 64), (2, 2)), -0.2, 0.2)), 0.5, 8.0)
    offsets = draw_offsets(jax.random.fold_in(streams_of[2], 71), 0)
    return {"coarse": coarse, "offsets": offsets}


def window(line, begin):
    return lax.dynamic_slice_in_dim(line, begin, line.shape[1] - 2 * HALO, 1)


def reference(coarse, offsets):
    padded = jnp.pad(coarse, ((0, 0), (0, 0), (HALO, HALO)))

    def spindown(column):
        starts = (HALO + column).astype(jnp.int32)
        shifted = jax.vmap(window)(padded, starts)
        return jnp.sum(shifted, axis=0) / SEGMENTS

    fine = lax.map(spindown, offsets.T)
    peaks = jnp.max(fine, axis=(0, 2))
    return fine, peaks
```

```python
import functools

import jax
import jax.numpy as jnp
from jax import lax
from jax.experimental import pallas as pl
from jax.experimental.pallas import tpu as pltpu
from jax.sharding import PartitionSpec as P

HALO = 8
LANES = 128


def accumulate(side_ref, offsets_ref, maps_ref, fine_ref, msg_ref, edge_ref, data, weights, total, in_sems, out_sems):
    seg_count = offsets_ref.shape[1]
    spin_count = offsets_ref.shape[0]
    points = maps_ref.shape[0] // seg_count
    tiles = maps_ref.shape[1] // LANES
    rows = spin_count * points
    groups = spin_count // 8

    def fetch(tile):
        return pltpu.make_async_copy(
            maps_ref.at[:, pl.ds(tile * LANES, LANES)], data.at[tile], in_sems.at[tile]
        )

    for tile in range(tiles):
        fetch(tile).start()
    for index in range(2 * HALO + 1):
        hit = offsets_ref[...] == index - HALO
        weights[pl.ds(index * spin_count, spin_count), :] = jnp.where(hit, 1.0 / seg_count, 0.0).astype(jnp.bfloat16)
    total[...] = jnp.zeros_like(total)

    lane = lax.broadcasted_iota(jnp.int32, (spin_count, LANES), 1)

    for pair in range(tiles // 2):
        fetch(2 * pair).wait()
        fetch(2 * pair + 1).wait()

        def point_step(point, carry, pair=pair):
            block = jnp.concatenate(
                [data.at[2 * pair + half][pl.ds(point, seg_count, stride=points), :] for half in range(2)],
                axis=1,
            )
            high = block.astype(jnp.bfloat16)
            low = (block - high.astype(jnp.float32)).astype(jnp.bfloat16)
            taps = weights[...]
            product = jnp.dot(taps, high, preferred_element_type=jnp.float32) + jnp.dot(
                taps, low, preferred_element_type=jnp.float32
            )
            sums = [jnp.zeros((spin_count, LANES), jnp.float32) for _ in range(4)]
            for index in range(2 * HALO + 1):
                shift = index - HALO
                part = product[index * spin_count : (index + 1) * spin_count]
                left, right = part[:, :LANES], part[:, LANES:]
                if shift == 0:
                    sums[1] = sums[1] + left
                    sums[2] = sums[2] + right
                    continue
                left = pltpu.roll(left, (-shift) % LANES, 1)
                right = pltpu.roll(right, (-shift) % LANES, 1)
                if shift > 0:
                    same = lane < LANES - shift
                    sums[0] = sums[0] + jnp.where(same, 0.0, left)
                    sums[1] = sums[1] + jnp.where(same, left, right)
                    sums[2] = sums[2] + jnp.where(same, right, 0.0)
                else:
                    same = lane >= -shift
                    sums[1] = sums[1] + jnp.where(same, left, 0.0)
                    sums[2] = sums[2] + jnp.where(same, right, left)
                    sums[3] = sums[3] + jnp.where(same, 0.0, right)
            for place in range(4):
                target = total.at[2 * pair + place]
                for group in range(groups):
                    where = pl.ds(group * 8 * points + point, 8, stride=points)
                    target[where, :] = target[where, :] + sums[place][group * 8 : group * 8 + 8]
            return carry

        lax.fori_loop(0, points, point_step, 0)

    def emit(tile):
        return pltpu.make_async_copy(
            total.at[tile + 1], fine_ref.at[:, pl.ds(tile * LANES, LANES)], out_sems.at[tile]
        )

    for tile in range(1, tiles - 1):
        emit(tile).start()
    side = side_ref[0]
    low_side = side == 0
    row_lane = lax.broadcasted_iota(jnp.int32, (points, LANES), 1)
    outer = row_lane >= LANES - HALO
    inner = row_lane < HALO
    best = jnp.full((points, LANES), -jnp.inf, jnp.float32)
    for spin in range(spin_count):
        where = pl.ds(spin * points, points)
        for tile in range(1, tiles - 1):
            best = jnp.maximum(best, total[tile + 1, where, :])
        first, last = total[1, where, :], total[tiles, where, :]
        best = jnp.maximum(best, jnp.where(row_lane < HALO * side, -jnp.inf, first))
        best = jnp.maximum(best, jnp.where(row_lane >= LANES - HALO * (1 - side), -jnp.inf, last))
    msg_ref[pl.ds(groups * points, points), :] = best
    for group in range(groups):
        packed = jnp.zeros((points, LANES), jnp.float32)
        for slot in range(8):
            where = pl.ds((group * 8 + slot) * points, points)
            first, last = total[1, where, :], total[tiles, where, :]
            before, after = total[0, where, :], total[tiles + 1, where, :]
            mine = jnp.where(
                low_side, jnp.where(inner, after, last), jnp.where(inner, first, before)
            )
            mine = jnp.where(jnp.logical_or(inner, outer), mine, 0.0)
            packed = packed + pltpu.roll(mine, (HALO + 2 * HALO * slot) % LANES, 1)
        msg_ref[pl.ds(group * points, points), :] = packed
    edge_ref[...] = jnp.where(low_side, total[tiles], total[1])

    @pl.when(low_side)
    def _():
        emit(0).start()
        emit(0).wait()

    @pl.when(jnp.logical_not(low_side))
    def _():
        emit(tiles - 1).start()
        emit(tiles - 1).wait()

    for tile in range(1, tiles - 1):
        emit(tile).wait()


def finish(side_ref, mine_ref, theirs_ref, edge_ref, fine_in, fine_ref, peaks_ref, block, sem):
    points = peaks_ref.shape[1]
    groups = mine_ref.shape[0] // points - 1
    tiles = fine_ref.shape[1] // LANES
    side = side_ref[0]
    low_side = side == 0
    row_lane = lax.broadcasted_iota(jnp.int32, (points, LANES), 1)
    start = jnp.where(low_side, LANES - HALO, 0)
    edge = jnp.logical_and(row_lane >= start, row_lane < start + HALO)
    tail = pl.ds(groups * points, points)
    best = jnp.maximum(mine_ref[tail, :], theirs_ref[tail, :])
    for group in range(groups):
        where = pl.ds(group * points, points)
        packed = mine_ref[where, :] + theirs_ref[where, :]
        best = jnp.maximum(best, packed)
        for slot in range(8):
            rows = pl.ds((group * 8 + slot) * points, points)
            back = pltpu.roll(packed, (-(HALO + 2 * HALO * slot)) % LANES, 1)
            block[rows, :] = jnp.where(edge, back, edge_ref[rows, :])
    tile = jnp.where(low_side, tiles - 1, 0)
    copy = pltpu.make_async_copy(
        block, fine_ref.at[:, pl.ds(pl.multiple_of(tile * LANES, LANES), LANES)], sem
    )
    copy.start()
    top = jnp.max(best, axis=1, keepdims=True)
    row = lax.broadcasted_iota(jnp.int32, (points, LANES), 0)
    spread = jnp.max(jnp.where(row == row_lane, top, -jnp.inf), axis=0, keepdims=True)
    peaks_ref[...] = spread[:, :points]
    copy.wait()


def on_device(coarse, offsets):
    nseg = lax.axis_size("seg")
    side = lax.axis_index("freq").astype(jnp.int32).reshape(1)
    local_segs, points_all, bins = coarse.shape
    points = points_all // nseg
    segs = local_segs * nseg
    spins = offsets.shape[1]
    tiles = bins // LANES
    rows = spins * points
    groups = spins // 8
    blocks = coarse.reshape(local_segs, nseg, points, bins).transpose(1, 0, 2, 3)
    maps = lax.all_to_all(blocks, "seg", split_axis=0, concat_axis=0, tiled=True)
    smem = pl.BlockSpec(memory_space=pltpu.SMEM)
    vmem = pl.BlockSpec(memory_space=pltpu.VMEM)
    anywhere = pl.BlockSpec(memory_space=pl.ANY)
    fine, mine, edge = pl.pallas_call(
        accumulate,
        out_shape=(
            jax.ShapeDtypeStruct((rows, bins), jnp.float32),
            jax.ShapeDtypeStruct(((groups + 1) * points, LANES), jnp.float32),
            jax.ShapeDtypeStruct((rows, LANES), jnp.float32),
        ),
        in_specs=[smem, vmem, anywhere],
        out_specs=(anywhere, vmem, vmem),
        scratch_shapes=[
            pltpu.VMEM((tiles, segs * points, LANES), jnp.float32),
            pltpu.VMEM(((2 * HALO + 1) * spins, segs), jnp.bfloat16),
            pltpu.VMEM((tiles + 2, rows, LANES), jnp.float32),
            pltpu.SemaphoreType.DMA((tiles,)),
            pltpu.SemaphoreType.DMA((tiles,)),
        ],
        compiler_params=pltpu.CompilerParams(vmem_limit_bytes=40 * 1024 * 1024),
        name="accumulate",
    )(side, offsets.T, maps.reshape(segs * points, bins))
    theirs = lax.ppermute(mine, "freq", [(0, 1), (1, 0)])
    fine, peaks = pl.pallas_call(
        finish,
        out_shape=(
            jax.ShapeDtypeStruct((rows, bins), jnp.float32),
            jax.ShapeDtypeStruct((1, points), jnp.float32),
        ),
        in_specs=[smem, vmem, vmem, vmem, anywhere],
        out_specs=(anywhere, vmem),
        scratch_shapes=[pltpu.VMEM((rows, LANES), jnp.float32), pltpu.SemaphoreType.DMA],
        input_output_aliases={4: 0},
        name="finish",
    )(side, mine, theirs, edge, fine)
    return fine.reshape(spins, points, bins), peaks.reshape(points)


def solution(mesh):
    return jax.shard_map(
        on_device,
        mesh=mesh,
        in_specs=(P("seg", None, "freq"), P()),
        out_specs=(P(None, "seg", "freq"), P("seg")),
        check_vma=False,
    )
```

```python
import jax
import jax.numpy as jnp
from jax import lax
from jax.experimental import pallas as pl
from jax.experimental.pallas import tpu as pltpu
from jax.sharding import PartitionSpec as P

HALO = 8
LANES = 128
SHIFTS = 2 * HALO + 1
OUTER, MIDDLE = 4, 2


def exchange_order(count):
    inner = count // (OUTER * MIDDLE)
    return [
        (outer * MIDDLE + middle) * inner + place
        for outer in range(OUTER)
        for place in range(inner)
        for middle in range(MIDDLE)
    ]


def pack(offsets_ref, coarse_ref, blocks_ref, taps_ref, sems):
    local, outer, middle, inner = coarse_ref.shape[:4]
    spin_count, seg_count = offsets_ref.shape
    copies = [
        pltpu.make_async_copy(coarse_ref.at[s, :, m], blocks_ref.at[:, :, m, s], sems.at[s, m])
        for s in range(local)
        for m in range(middle)
    ]
    for copy in copies:
        copy.start()
    source = lax.broadcasted_iota(jnp.int32, (seg_count, seg_count), 0)
    arrival = lax.broadcasted_iota(jnp.int32, (seg_count, seg_count), 1)
    device, s = arrival // local, arrival % local
    m, rest = device % middle, device // middle
    natural = (((rest // inner) * middle + m) * inner + rest % inner) * local + s
    move = jnp.where(source == natural, 1.0, 0.0).astype(jnp.bfloat16)
    arrived = jnp.dot(
        offsets_ref[...].astype(jnp.float32).astype(jnp.bfloat16), move, preferred_element_type=jnp.float32
    )
    for index in range(SHIFTS):
        hit = arrived == float(index - HALO)
        taps_ref[pl.ds(index * spin_count, spin_count), :] = jnp.where(hit, 1.0 / seg_count, 0.0).astype(jnp.bfloat16)
    for copy in copies:
        copy.wait()


def accumulate(taps_ref, maps_ref, fine_ref, msg_ref, rest_ref, data, total, in_sems, out_sems):
    seg_count = taps_ref.shape[1]
    spin_count = taps_ref.shape[0] // SHIFTS
    points = maps_ref.shape[0] // seg_count
    tiles = maps_ref.shape[1] // LANES
    pairs = tiles // 2
    groups = spin_count // 8

    def fetch(tile):
        return pltpu.make_async_copy(
            maps_ref.at[:, pl.ds(tile * LANES, LANES)], data.at[tile], in_sems.at[tile]
        )

    def emit(tile):
        return pltpu.make_async_copy(
            total.at[tile + 1], fine_ref.at[:, pl.ds(tile * LANES, LANES)], out_sems.at[tile]
        )

    for tile in range(4):
        fetch(tile).start()
    total[...] = jnp.zeros_like(total)
    lane = lax.broadcasted_iota(jnp.int32, (spin_count, LANES), 1)

    for pair in range(pairs):
        fetch(2 * pair).wait()
        fetch(2 * pair + 1).wait()
        if pair + 2 < pairs:
            fetch(2 * pair + 4).start()
            fetch(2 * pair + 5).start()

        def point_step(point, carry, pair=pair):
            block = jnp.concatenate(
                [data.at[2 * pair + half][pl.ds(point, seg_count, stride=points), :] for half in range(2)],
                axis=1,
            )
            high = block.astype(jnp.bfloat16)
            low = (block - high.astype(jnp.float32)).astype(jnp.bfloat16)
            taps = taps_ref[...]
            product = jnp.dot(taps, high, preferred_element_type=jnp.float32) + jnp.dot(
                taps, low, preferred_element_type=jnp.float32
            )
            sums = [jnp.zeros((spin_count, LANES), jnp.float32) for _ in range(4)]
            for index in range(SHIFTS):
                shift = index - HALO
                part = product[index * spin_count : (index + 1) * spin_count]
                left, right = part[:, :LANES], part[:, LANES:]
                if shift == 0:
                    sums[1] = sums[1] + left
                    sums[2] = sums[2] + right
                    continue
                left = pltpu.roll(left, (-shift) % LANES, 1)
                right = pltpu.roll(right, (-shift) % LANES, 1)
                if shift > 0:
                    same = lane < LANES - shift
                    sums[0] = sums[0] + jnp.where(same, 0.0, left)
                    sums[1] = sums[1] + jnp.where(same, left, right)
                    sums[2] = sums[2] + jnp.where(same, right, 0.0)
                else:
                    same = lane >= -shift
                    sums[1] = sums[1] + jnp.where(same, left, 0.0)
                    sums[2] = sums[2] + jnp.where(same, right, left)
                    sums[3] = sums[3] + jnp.where(same, 0.0, right)
            for place in range(4):
                target = total.at[2 * pair + place]
                for group in range(groups):
                    where = pl.ds(group * 8 * points + point, 8, stride=points)
                    target[where, :] = target[where, :] + sums[place][group * 8 : group * 8 + 8]
            return carry

        lax.fori_loop(0, points, point_step, 0, unroll=4)
        if pair + 1 < pairs:
            for tile in range(max(1, 2 * pair - 1), 2 * pair + 1):
                emit(tile).start()

    side = lax.axis_index("freq")
    low_side = side == 0
    row_lane = lax.broadcasted_iota(jnp.int32, (points, LANES), 1)
    outer = row_lane >= LANES - HALO
    inner = row_lane < HALO
    best = jnp.full((points, LANES), -jnp.inf, jnp.float32)
    for spin in range(spin_count):
        where = pl.ds(spin * points, points)
        for tile in range(1, tiles - 1):
            best = jnp.maximum(best, total[tile + 1, where, :])
        first, last = total[1, where, :], total[tiles, where, :]
        best = jnp.maximum(best, jnp.where(row_lane < HALO * side, -jnp.inf, first))
        best = jnp.maximum(best, jnp.where(row_lane >= LANES - HALO * (1 - side), -jnp.inf, last))
    msg_ref[pl.ds(groups * points, points), :] = best
    for group in range(groups):
        packed = jnp.zeros((points, LANES), jnp.float32)
        for slot in range(8):
            where = pl.ds((group * 8 + slot) * points, points)
            first, last = total[1, where, :], total[tiles, where, :]
            before, after = total[0, where, :], total[tiles + 1, where, :]
            mine = jnp.where(
                low_side, jnp.where(inner, after, last), jnp.where(inner, first, before)
            )
            mine = jnp.where(jnp.logical_or(inner, outer), mine, 0.0)
            packed = packed + pltpu.roll(mine, (HALO + 2 * HALO * slot) % LANES, 1)
        msg_ref[pl.ds(group * points, points), :] = packed
    rest_ref[0] = total[1]
    for place in range(3):
        rest_ref[1 + place] = total[tiles - 2 + place]
    for tile in range(1, tiles - 3):
        emit(tile).wait()


def finish(mine_ref, theirs_ref, rest_ref, fine_in, fine_ref, peaks_ref, first, last, sems):
    points = peaks_ref.shape[1]
    groups = mine_ref.shape[0] // points - 1
    tiles = fine_ref.shape[1] // LANES

    def emit(source, tile, place):
        return pltpu.make_async_copy(source, fine_ref.at[:, pl.ds(tile * LANES, LANES)], sems.at[place])

    copies = [
        emit(first, 0, 0),
        emit(rest_ref.at[1], tiles - 3, 1),
        emit(rest_ref.at[2], tiles - 2, 2),
        emit(last, tiles - 1, 3),
    ]
    copies[1].start()
    copies[2].start()
    side = lax.axis_index("freq")
    row_lane = lax.broadcasted_iota(jnp.int32, (points, LANES), 1)
    tail = pl.ds(groups * points, points)
    best = jnp.maximum(mine_ref[tail, :], theirs_ref[tail, :])
    for group in range(groups):
        where = pl.ds(group * points, points)
        packed = mine_ref[where, :] + theirs_ref[where, :]
        best = jnp.maximum(best, packed)
        for slot in range(8):
            rows = pl.ds((group * 8 + slot) * points, points)
            back = pltpu.roll(packed, (-(HALO + 2 * HALO * slot)) % LANES, 1)
            first[rows, :] = jnp.where(row_lane < HALO * side, back, rest_ref[0, rows, :])
            last[rows, :] = jnp.where(row_lane >= LANES - HALO * (1 - side), back, rest_ref[3, rows, :])
    copies[0].start()
    copies[3].start()
    top = jnp.max(best, axis=1, keepdims=True)
    row = lax.broadcasted_iota(jnp.int32, (points, LANES), 0)
    spread = jnp.max(jnp.where(row == row_lane, top, -jnp.inf), axis=0, keepdims=True)
    peaks_ref[...] = spread[:, :points]
    for copy in copies:
        copy.wait()


def on_device(coarse, offsets):
    nseg = lax.axis_size("seg")
    local_segs, points_all, bins = coarse.shape
    points = points_all // nseg
    segs = local_segs * nseg
    spins = offsets.shape[1]
    tiles = bins // LANES
    rows = spins * points
    groups = spins // 8
    inner = nseg // (OUTER * MIDDLE)
    vmem = pl.BlockSpec(memory_space=pltpu.VMEM)
    anywhere = pl.BlockSpec(memory_space=pl.ANY)
    mib = 1024 * 1024
    blocks, taps = pl.pallas_call(
        pack,
        out_shape=(
            jax.ShapeDtypeStruct((OUTER, inner, MIDDLE, local_segs, points, bins), jnp.float32),
            jax.ShapeDtypeStruct((SHIFTS * spins, segs), jnp.bfloat16),
        ),
        in_specs=[vmem, pl.BlockSpec(memory_space=pltpu.HBM)],
        out_specs=(vmem, vmem),
        scratch_shapes=[pltpu.SemaphoreType.DMA((local_segs, MIDDLE))],
        compiler_params=pltpu.CompilerParams(vmem_limit_bytes=16 * mib),
        name="pack",
    )(offsets.T, coarse.reshape(local_segs, OUTER, MIDDLE, inner, points, bins))
    maps = lax.all_to_all(
        blocks.reshape(nseg, local_segs, points, bins),
        "seg",
        split_axis=0,
        concat_axis=0,
        tiled=True,
        axis_index_groups=[exchange_order(nseg)],
    )
    fine, mine, rest = pl.pallas_call(
        accumulate,
        out_shape=(
            jax.ShapeDtypeStruct((rows, bins), jnp.float32),
            jax.ShapeDtypeStruct(((groups + 1) * points, LANES), jnp.float32),
            jax.ShapeDtypeStruct((4, rows, LANES), jnp.float32),
        ),
        in_specs=[vmem, anywhere],
        out_specs=(anywhere, vmem, vmem),
        scratch_shapes=[
            pltpu.VMEM((tiles, segs * points, LANES), jnp.float32),
            pltpu.VMEM((tiles + 2, rows, LANES), jnp.float32),
            pltpu.SemaphoreType.DMA((tiles,)),
            pltpu.SemaphoreType.DMA((tiles,)),
        ],
        compiler_params=pltpu.CompilerParams(vmem_limit_bytes=24 * mib),
        name="accumulate",
    )(taps, maps.reshape(segs * points, bins))
    theirs = lax.ppermute(mine, "freq", [(0, 1), (1, 0)])
    fine, peaks = pl.pallas_call(
        finish,
        out_shape=(
            jax.ShapeDtypeStruct((rows, bins), jnp.float32),
            jax.ShapeDtypeStruct((1, points), jnp.float32),
        ),
        in_specs=[vmem, vmem, vmem, anywhere],
        out_specs=(anywhere, vmem),
        scratch_shapes=[
            pltpu.VMEM((rows, LANES), jnp.float32),
            pltpu.VMEM((rows, LANES), jnp.float32),
            pltpu.SemaphoreType.DMA((4,)),
        ],
        input_output_aliases={3: 0},
        compiler_params=pltpu.CompilerParams(vmem_limit_bytes=4 * mib),
        name="finish",
    )(mine, theirs, rest, fine)
    return fine.reshape(spins, points, bins), peaks.reshape(points)


def solution(mesh):
    return jax.shard_map(
        on_device,
        mesh=mesh,
        in_specs=(P("seg", None, "freq"), P()),
        out_specs=(P(None, "seg", "freq"), P("seg")),
        check_vma=False,
    )
```

```python
import functools

import jax
import jax.numpy as jnp
from jax import lax
from jax.experimental import pallas as pl
from jax.experimental.pallas import tpu as pltpu
from jax.sharding import PartitionSpec as P

HALO = 8
LANES = 128
SHIFTS = 2 * HALO + 1
OUTER, MIDDLE = 4, 2


def exchange_order(count):
    inner = count // (OUTER * MIDDLE)
    return [
        (outer * MIDDLE + middle) * inner + place
        for outer in range(OUTER)
        for place in range(inner)
        for middle in range(MIDDLE)
    ]


def pack(coarse_ref, blocks_ref, sems):
    local, outer, middle, inner = coarse_ref.shape[:4]
    copies = [
        pltpu.make_async_copy(coarse_ref.at[s, :, m], blocks_ref.at[:, :, m, s], sems.at[s, m])
        for s in range(local)
        for m in range(middle)
    ]
    for copy in copies:
        copy.start()
    for copy in copies:
        copy.wait()


def write_taps(local, offsets_ref, taps_ref):
    spin_count, seg_count = offsets_ref.shape
    middle, inner = MIDDLE, seg_count // local // (OUTER * MIDDLE)
    source = lax.broadcasted_iota(jnp.int32, (seg_count, seg_count), 0)
    arrival = lax.broadcasted_iota(jnp.int32, (seg_count, seg_count), 1)
    device, s = arrival // local, arrival % local
    m, rest = device % middle, device // middle
    natural = (((rest // inner) * middle + m) * inner + rest % inner) * local + s
    move = jnp.where(source == natural, 1.0, 0.0).astype(jnp.bfloat16)
    arrived = jnp.dot(
        offsets_ref[...].astype(jnp.float32).astype(jnp.bfloat16), move, preferred_element_type=jnp.float32
    )
    for index in range(SHIFTS):
        hit = arrived == float(index - HALO)
        taps_ref[pl.ds(index * spin_count, spin_count), :] = jnp.where(hit, 1.0 / seg_count, 0.0).astype(jnp.bfloat16)


def accumulate(local, offsets_ref, maps_ref, fine_ref, msg_ref, rest_ref, data, taps_ref, total, early, late, in_sems, out_sems):
    spin_count, seg_count = offsets_ref.shape
    points = maps_ref.shape[0] // seg_count
    tiles = maps_ref.shape[1] // LANES
    pairs = tiles // 2
    groups = spin_count // 8

    def fetch(tile):
        return pltpu.make_async_copy(
            maps_ref.at[:, pl.ds(tile * LANES, LANES)], data.at[tile], in_sems.at[tile]
        )

    def emit(tile):
        return pltpu.make_async_copy(
            total.at[tile + 1], fine_ref.at[:, pl.ds(tile * LANES, LANES)], out_sems.at[tile]
        )

    for tile in range(4):
        fetch(tile).start()
    write_taps(local, offsets_ref, taps_ref)
    total[...] = jnp.zeros_like(total)
    lane = lax.broadcasted_iota(jnp.int32, (spin_count, LANES), 1)

    def multiply(pair, point, product):
        block = jnp.concatenate(
            [data.at[2 * pair + half][pl.ds(point, seg_count, stride=points), :] for half in range(2)],
            axis=1,
        )
        high = block.astype(jnp.bfloat16)
        low = (block - high.astype(jnp.float32)).astype(jnp.bfloat16)
        taps = taps_ref[...]
        product[...] = jnp.dot(taps, high, preferred_element_type=jnp.float32) + jnp.dot(
            taps, low, preferred_element_type=jnp.float32
        )

    def combine(pair, point, product):
        sums = [jnp.zeros((spin_count, LANES), jnp.float32) for _ in range(4)]
        for index in range(SHIFTS):
            shift = index - HALO
            where = pl.ds(index * spin_count, spin_count)
            left, right = product[where, :LANES], product[where, LANES:]
            if shift == 0:
                sums[1] = sums[1] + left
                sums[2] = sums[2] + right
                continue
            left = pltpu.roll(left, (-shift) % LANES, 1)
            right = pltpu.roll(right, (-shift) % LANES, 1)
            if shift > 0:
                same = lane < LANES - shift
                sums[0] = sums[0] + jnp.where(same, 0.0, left)
                sums[1] = sums[1] + jnp.where(same, left, right)
                sums[2] = sums[2] + jnp.where(same, right, 0.0)
            else:
                same = lane >= -shift
                sums[1] = sums[1] + jnp.where(same, left, 0.0)
                sums[2] = sums[2] + jnp.where(same, right, left)
                sums[3] = sums[3] + jnp.where(same, 0.0, right)
        for place in range(4):
            target = total.at[2 * pair + place]
            for group in range(groups):
                where = pl.ds(group * 8 * points + point, 8, stride=points)
                target[where, :] = target[where, :] + sums[place][group * 8 : group * 8 + 8]

    def arrive(pair):
        fetch(2 * pair).wait()
        fetch(2 * pair + 1).wait()
        if pair + 2 < pairs:
            fetch(2 * pair + 4).start()
            fetch(2 * pair + 5).start()

    half = points // 2
    arrive(0)
    for point in range(half):
        multiply(0, point, early.at[point])
    for pair in range(pairs):
        if pair + 1 < pairs:
            arrive(pair + 1)
        for point in range(half):
            multiply(pair, half + point, late.at[point])
            combine(pair, point, early.at[point])
        for point in range(half):
            if pair + 1 < pairs:
                multiply(pair + 1, point, early.at[point])
            combine(pair, half + point, late.at[point])
        if pair + 1 < pairs:
            for tile in range(max(1, 2 * pair - 1), 2 * pair + 1):
                emit(tile).start()

    side = lax.axis_index("freq")
    low_side = side == 0
    row_lane = lax.broadcasted_iota(jnp.int32, (points, LANES), 1)
    outer = row_lane >= LANES - HALO
    inner = row_lane < HALO
    best = jnp.full((points, LANES), -jnp.inf, jnp.float32)
    for spin in range(spin_count):
        where = pl.ds(spin * points, points)
        for tile in range(1, tiles - 1):
            best = jnp.maximum(best, total[tile + 1, where, :])
        first, last = total[1, where, :], total[tiles, where, :]
        best = jnp.maximum(best, jnp.where(row_lane < HALO * side, -jnp.inf, first))
        best = jnp.maximum(best, jnp.where(row_lane >= LANES - HALO * (1 - side), -jnp.inf, last))
    msg_ref[pl.ds(groups * points, points), :] = best
    for group in range(groups):
        packed = jnp.zeros((points, LANES), jnp.float32)
        for slot in range(8):
            where = pl.ds((group * 8 + slot) * points, points)
            first, last = total[1, where, :], total[tiles, where, :]
            before, after = total[0, where, :], total[tiles + 1, where, :]
            mine = jnp.where(
                low_side, jnp.where(inner, after, last), jnp.where(inner, first, before)
            )
            mine = jnp.where(jnp.logical_or(inner, outer), mine, 0.0)
            packed = packed + pltpu.roll(mine, (HALO + 2 * HALO * slot) % LANES, 1)
        msg_ref[pl.ds(group * points, points), :] = packed
    rest_ref[0] = total[1]
    for place in range(3):
        rest_ref[1 + place] = total[tiles - 2 + place]
    for tile in range(1, tiles - 3):
        emit(tile).wait()


def finish(mine_ref, theirs_ref, rest_ref, fine_in, fine_ref, peaks_ref, first, last, sems):
    points = peaks_ref.shape[1]
    groups = mine_ref.shape[0] // points - 1
    tiles = fine_ref.shape[1] // LANES

    def emit(source, tile, place):
        return pltpu.make_async_copy(source, fine_ref.at[:, pl.ds(tile * LANES, LANES)], sems.at[place])

    copies = [
        emit(first, 0, 0),
        emit(rest_ref.at[1], tiles - 3, 1),
        emit(rest_ref.at[2], tiles - 2, 2),
        emit(last, tiles - 1, 3),
    ]
    copies[1].start()
    copies[2].start()
    side = lax.axis_index("freq")
    row_lane = lax.broadcasted_iota(jnp.int32, (points, LANES), 1)
    tail = pl.ds(groups * points, points)
    best = jnp.maximum(mine_ref[tail, :], theirs_ref[tail, :])
    for group in range(groups):
        where = pl.ds(group * points, points)
        packed = mine_ref[where, :] + theirs_ref[where, :]
        best = jnp.maximum(best, packed)
        for slot in range(8):
            rows = pl.ds((group * 8 + slot) * points, points)
            back = pltpu.roll(packed, (-(HALO + 2 * HALO * slot)) % LANES, 1)
            first[rows, :] = jnp.where(row_lane < HALO * side, back, rest_ref[0, rows, :])
            last[rows, :] = jnp.where(row_lane >= LANES - HALO * (1 - side), back, rest_ref[3, rows, :])
    copies[0].start()
    copies[3].start()
    top = jnp.max(best, axis=1, keepdims=True)
    row = lax.broadcasted_iota(jnp.int32, (points, LANES), 0)
    spread = jnp.max(jnp.where(row == row_lane, top, -jnp.inf), axis=0, keepdims=True)
    peaks_ref[...] = spread[:, :points]
    for copy in copies:
        copy.wait()


def on_device(coarse, offsets):
    nseg = lax.axis_size("seg")
    local_segs, points_all, bins = coarse.shape
    points = points_all // nseg
    segs = local_segs * nseg
    spins = offsets.shape[1]
    tiles = bins // LANES
    rows = spins * points
    groups = spins // 8
    inner = nseg // (OUTER * MIDDLE)
    vmem = pl.BlockSpec(memory_space=pltpu.VMEM)
    anywhere = pl.BlockSpec(memory_space=pl.ANY)
    mib = 1024 * 1024
    blocks = pl.pallas_call(
        pack,
        out_shape=jax.ShapeDtypeStruct((OUTER, inner, MIDDLE, local_segs, points, bins), jnp.float32),
        in_specs=[anywhere],
        out_specs=vmem,
        scratch_shapes=[pltpu.SemaphoreType.DMA((local_segs, MIDDLE))],
        compiler_params=pltpu.CompilerParams(vmem_limit_bytes=44 * mib),
        name="pack",
    )(coarse.reshape(local_segs, OUTER, MIDDLE, inner, points, bins))
    maps = lax.all_to_all(
        blocks.reshape(nseg, local_segs, points, bins),
        "seg",
        split_axis=0,
        concat_axis=0,
        tiled=True,
        axis_index_groups=[exchange_order(nseg)],
    )
    fine, mine, rest = pl.pallas_call(
        functools.partial(accumulate, local_segs),
        out_shape=(
            jax.ShapeDtypeStruct((rows, bins), jnp.float32),
            jax.ShapeDtypeStruct(((groups + 1) * points, LANES), jnp.float32),
            jax.ShapeDtypeStruct((4, rows, LANES), jnp.float32),
        ),
        in_specs=[vmem, anywhere],
        out_specs=(anywhere, vmem, vmem),
        scratch_shapes=[
            pltpu.VMEM((tiles, segs * points, LANES), jnp.float32),
            pltpu.VMEM((SHIFTS * spins, segs), jnp.bfloat16),
            pltpu.VMEM((tiles + 2, rows, LANES), jnp.float32),
            pltpu.VMEM((points // 2, SHIFTS * spins, 2 * LANES), jnp.float32),
            pltpu.VMEM((points // 2, SHIFTS * spins, 2 * LANES), jnp.float32),
            pltpu.SemaphoreType.DMA((tiles,)),
            pltpu.SemaphoreType.DMA((tiles,)),
        ],
        compiler_params=pltpu.CompilerParams(vmem_limit_bytes=24 * mib),
        name="accumulate",
    )(offsets.T, maps.reshape(segs * points, bins))
    theirs = lax.ppermute(mine, "freq", [(0, 1), (1, 0)])
    fine, peaks = pl.pallas_call(
        finish,
        out_shape=(
            jax.ShapeDtypeStruct((rows, bins), jnp.float32),
            jax.ShapeDtypeStruct((1, points), jnp.float32),
        ),
        in_specs=[vmem, vmem, vmem, anywhere],
        out_specs=(anywhere, vmem),
        scratch_shapes=[
            pltpu.VMEM((rows, LANES), jnp.float32),
            pltpu.VMEM((rows, LANES), jnp.float32),
            pltpu.SemaphoreType.DMA((4,)),
        ],
        input_output_aliases={3: 0},
        compiler_params=pltpu.CompilerParams(vmem_limit_bytes=4 * mib),
        name="finish",
    )(mine, theirs, rest, fine)
    return fine.reshape(spins, points, bins), peaks.reshape(points)


def solution(mesh):
    return jax.shard_map(
        on_device,
        mesh=mesh,
        in_specs=(P("seg", None, "freq"), P()),
        out_specs=(P(None, "seg", "freq"), P("seg")),
        check_vma=False,
    )
```

```python
import functools

import jax
import jax.numpy as jnp
from jax import lax
from jax.experimental import pallas as pl
from jax.experimental.pallas import tpu as pltpu
from jax.sharding import PartitionSpec as P

HALO = 8
LANES = 128
SHIFTS = 2 * HALO + 1
ALONG = (4, 2, 4, 2)


def exchange_order():
    ys, zs, xs, cores = ALONG
    return [
        ((y * zs + z) * xs + x) * cores + core
        for core in range(cores)
        for z in range(zs)
        for y in range(ys)
        for x in range(xs)
    ]


def pack(coarse_ref, blocks_ref, sems):
    local, _, zs, _, cores = coarse_ref.shape[:5]
    copies = [
        pltpu.make_async_copy(
            coarse_ref.at[s, :, z, :, core], blocks_ref.at[core, z, :, :, s], sems.at[s, z, core]
        )
        for s in range(local)
        for z in range(zs)
        for core in range(cores)
    ]
    for copy in copies:
        copy.start()
    for copy in copies:
        copy.wait()


def write_taps(local, offsets_ref, taps_ref):
    spin_count, seg_count = offsets_ref.shape
    ys, zs, xs, cores = ALONG
    source = lax.broadcasted_iota(jnp.int32, (seg_count, seg_count), 0)
    arrival = lax.broadcasted_iota(jnp.int32, (seg_count, seg_count), 1)
    s, device = arrival % local, arrival // local
    x, device = device % xs, device // xs
    y, device = device % ys, device // ys
    z, core = device % zs, device // zs
    natural = (((y * zs + z) * xs + x) * cores + core) * local + s
    move = jnp.where(source == natural, 1.0, 0.0).astype(jnp.bfloat16)
    arrived = jnp.dot(
        offsets_ref[...].astype(jnp.float32).astype(jnp.bfloat16), move, preferred_element_type=jnp.float32
    )
    for index in range(SHIFTS):
        hit = arrived == float(index - HALO)
        taps_ref[pl.ds(index * spin_count, spin_count), :] = jnp.where(hit, 1.0 / seg_count, 0.0).astype(jnp.bfloat16)


def accumulate(local, offsets_ref, maps_ref, fine_ref, msg_ref, rest_ref, data, taps_ref, total, early, late, in_sem, out_sems):
    spin_count, seg_count = offsets_ref.shape
    points = maps_ref.shape[0] // seg_count
    tiles = maps_ref.shape[1] // LANES
    pairs = tiles // 2
    groups = spin_count // 8

    def fetch(tile):
        return pltpu.make_async_copy(
            maps_ref.at[:, pl.ds(tile * LANES, LANES)], data.at[tile], in_sem
        )

    def take(tile):
        for row in range(0, seg_count * points, 8 * points):
            data[tile, pl.ds(row, 8 * points), :] = maps_ref[pl.ds(row, 8 * points), tile * LANES : (tile + 1) * LANES]

    def emit(tile):
        return pltpu.make_async_copy(
            total.at[tile + 1], fine_ref.at[:, pl.ds(tile * LANES, LANES)], out_sems.at[tile]
        )

    take(0)
    take(1)
    write_taps(local, offsets_ref, taps_ref)
    total[...] = jnp.zeros_like(total)
    lane = lax.broadcasted_iota(jnp.int32, (spin_count, LANES), 1)

    def multiply(pair, point, product):
        block = jnp.concatenate(
            [data.at[2 * pair + half][pl.ds(point, seg_count, stride=points), :] for half in range(2)],
            axis=1,
        )
        high = block.astype(jnp.bfloat16)
        low = (block - high.astype(jnp.float32)).astype(jnp.bfloat16)
        taps = taps_ref[...]
        product[...] = jnp.dot(taps, high, preferred_element_type=jnp.float32) + jnp.dot(
            taps, low, preferred_element_type=jnp.float32
        )

    def combine(pair, point, product):
        sums = [jnp.zeros((spin_count, LANES), jnp.float32) for _ in range(4)]
        for index in range(SHIFTS):
            shift = index - HALO
            where = pl.ds(index * spin_count, spin_count)
            left, right = product[where, :LANES], product[where, LANES:]
            if shift == 0:
                sums[1] = sums[1] + left
                sums[2] = sums[2] + right
                continue
            left = pltpu.roll(left, (-shift) % LANES, 1)
            right = pltpu.roll(right, (-shift) % LANES, 1)
            if shift > 0:
                same = lane < LANES - shift
                sums[0] = sums[0] + jnp.where(same, 0.0, left)
                sums[1] = sums[1] + jnp.where(same, left, right)
                sums[2] = sums[2] + jnp.where(same, right, 0.0)
            else:
                same = lane >= -shift
                sums[1] = sums[1] + jnp.where(same, left, 0.0)
                sums[2] = sums[2] + jnp.where(same, right, left)
                sums[3] = sums[3] + jnp.where(same, 0.0, right)
        for place in range(4):
            target = total.at[2 * pair + place]
            for group in range(groups):
                where = pl.ds(group * 8 * points + point, 8, stride=points)
                target[where, :] = target[where, :] + sums[place][group * 8 : group * 8 + 8]

    half = points // 2
    for point in range(half):
        multiply(0, point, early.at[point])
    for tile in range(2, tiles - 1):
        take(tile)
    fetch(tiles - 1).start()
    fetch(tiles - 1).wait()
    for pair in range(pairs):
        for point in range(half):
            multiply(pair, half + point, late.at[point])
            combine(pair, point, early.at[point])
        for point in range(half):
            if pair + 1 < pairs:
                multiply(pair + 1, point, early.at[point])
            combine(pair, half + point, late.at[point])
        if pair + 1 < pairs:
            for tile in range(max(1, 2 * pair - 1), 2 * pair + 1):
                emit(tile).start()

    side = lax.axis_index("freq")
    low_side = side == 0
    row_lane = lax.broadcasted_iota(jnp.int32, (points, LANES), 1)
    outer = row_lane >= LANES - HALO
    inner = row_lane < HALO
    best = jnp.full((points, LANES), -jnp.inf, jnp.float32)
    for spin in range(spin_count):
        where = pl.ds(spin * points, points)
        for tile in range(1, tiles - 1):
            best = jnp.maximum(best, total[tile + 1, where, :])
        first, last = total[1, where, :], total[tiles, where, :]
        best = jnp.maximum(best, jnp.where(row_lane < HALO * side, -jnp.inf, first))
        best = jnp.maximum(best, jnp.where(row_lane >= LANES - HALO * (1 - side), -jnp.inf, last))
    msg_ref[pl.ds(groups * points, points), :] = best
    for group in range(groups):
        packed = jnp.zeros((points, LANES), jnp.float32)
        for slot in range(8):
            where = pl.ds((group * 8 + slot) * points, points)
            first, last = total[1, where, :], total[tiles, where, :]
            before, after = total[0, where, :], total[tiles + 1, where, :]
            mine = jnp.where(
                low_side, jnp.where(inner, after, last), jnp.where(inner, first, before)
            )
            mine = jnp.where(jnp.logical_or(inner, outer), mine, 0.0)
            packed = packed + pltpu.roll(mine, (HALO + 2 * HALO * slot) % LANES, 1)
        msg_ref[pl.ds(group * points, points), :] = packed
    rest_ref[0] = total[1]
    for place in range(3):
        rest_ref[1 + place] = total[tiles - 2 + place]
    for tile in range(1, tiles - 3):
        emit(tile).wait()


def finish(mine_ref, theirs_ref, rest_ref, fine_in, fine_ref, peaks_ref, first, last, sems):
    points = peaks_ref.shape[1]
    groups = mine_ref.shape[0] // points - 1
    tiles = fine_ref.shape[1] // LANES

    def emit(source, tile, place):
        return pltpu.make_async_copy(source, fine_ref.at[:, pl.ds(tile * LANES, LANES)], sems.at[place])

    copies = [
        emit(first, 0, 0),
        emit(rest_ref.at[1], tiles - 3, 1),
        emit(rest_ref.at[2], tiles - 2, 2),
        emit(last, tiles - 1, 3),
    ]
    copies[1].start()
    copies[2].start()
    side = lax.axis_index("freq")
    row_lane = lax.broadcasted_iota(jnp.int32, (points, LANES), 1)
    tail = pl.ds(groups * points, points)
    best = jnp.maximum(mine_ref[tail, :], theirs_ref[tail, :])
    for group in range(groups):
        where = pl.ds(group * points, points)
        packed = mine_ref[where, :] + theirs_ref[where, :]
        best = jnp.maximum(best, packed)
        for slot in range(8):
            rows = pl.ds((group * 8 + slot) * points, points)
            back = pltpu.roll(packed, (-(HALO + 2 * HALO * slot)) % LANES, 1)
            first[rows, :] = jnp.where(row_lane < HALO * side, back, rest_ref[0, rows, :])
            last[rows, :] = jnp.where(row_lane >= LANES - HALO * (1 - side), back, rest_ref[3, rows, :])
    copies[0].start()
    copies[3].start()
    top = jnp.max(best, axis=1, keepdims=True)
    row = lax.broadcasted_iota(jnp.int32, (points, LANES), 0)
    spread = jnp.max(jnp.where(row == row_lane, top, -jnp.inf), axis=0, keepdims=True)
    peaks_ref[...] = spread[:, :points]
    for copy in copies:
        copy.wait()


def on_device(coarse, offsets):
    nseg = lax.axis_size("seg")
    local_segs, points_all, bins = coarse.shape
    points = points_all // nseg
    segs = local_segs * nseg
    spins = offsets.shape[1]
    tiles = bins // LANES
    rows = spins * points
    groups = spins // 8
    ys, zs, xs, cores = ALONG
    vmem = pl.BlockSpec(memory_space=pltpu.VMEM)
    anywhere = pl.BlockSpec(memory_space=pl.ANY)
    mib = 1024 * 1024
    blocks = pl.pallas_call(
        pack,
        out_shape=jax.ShapeDtypeStruct((cores, zs, ys, xs, local_segs, points, bins), jnp.float32),
        in_specs=[anywhere],
        out_specs=vmem,
        scratch_shapes=[pltpu.SemaphoreType.DMA((local_segs, zs, cores))],
        compiler_params=pltpu.CompilerParams(vmem_limit_bytes=44 * mib),
        name="pack",
    )(coarse.reshape(local_segs, ys, zs, xs, cores, points, bins))
    maps = lax.all_to_all(
        blocks.reshape(nseg, local_segs, points, bins),
        "seg",
        split_axis=0,
        concat_axis=0,
        tiled=True,
        axis_index_groups=[exchange_order()],
    )
    fine, mine, rest = pl.pallas_call(
        functools.partial(accumulate, local_segs),
        out_shape=(
            jax.ShapeDtypeStruct((rows, bins), jnp.float32),
            jax.ShapeDtypeStruct(((groups + 1) * points, LANES), jnp.float32),
            jax.ShapeDtypeStruct((4, rows, LANES), jnp.float32),
        ),
        in_specs=[vmem, vmem],
        out_specs=(anywhere, vmem, vmem),
        scratch_shapes=[
            pltpu.VMEM((tiles, segs * points, LANES), jnp.float32),
            pltpu.VMEM((SHIFTS * spins, segs), jnp.bfloat16),
            pltpu.VMEM((tiles + 2, rows, LANES), jnp.float32),
            pltpu.VMEM((points // 2, SHIFTS * spins, 2 * LANES), jnp.float32),
            pltpu.VMEM((points // 2, SHIFTS * spins, 2 * LANES), jnp.float32),
            pltpu.SemaphoreType.DMA,
            pltpu.SemaphoreType.DMA((tiles,)),
        ],
        compiler_params=pltpu.CompilerParams(vmem_limit_bytes=24 * mib),
        name="accumulate",
    )(offsets.T, maps.reshape(segs * points, bins))
    theirs = lax.ppermute(mine, "freq", [(0, 1), (1, 0)])
    fine, peaks = pl.pallas_call(
        finish,
        out_shape=(
            jax.ShapeDtypeStruct((rows, bins), jnp.float32),
            jax.ShapeDtypeStruct((1, points), jnp.float32),
        ),
        in_specs=[vmem, vmem, vmem, anywhere],
        out_specs=(anywhere, vmem),
        scratch_shapes=[
            pltpu.VMEM((rows, LANES), jnp.float32),
            pltpu.VMEM((rows, LANES), jnp.float32),
            pltpu.SemaphoreType.DMA((4,)),
        ],
        input_output_aliases={3: 0},
        compiler_params=pltpu.CompilerParams(vmem_limit_bytes=4 * mib),
        name="finish",
    )(mine, theirs, rest, fine)
    return fine.reshape(spins, points, bins), peaks.reshape(points)


def solution(mesh):
    return jax.shard_map(
        on_device,
        mesh=mesh,
        in_specs=(P("seg", None, "freq"), P()),
        out_specs=(P(None, "seg", "freq"), P("seg")),
        check_vma=False,
    )
```

```python
import functools

import jax
import jax.numpy as jnp
from jax import lax
from jax.experimental import pallas as pl
from jax.experimental.pallas import tpu as pltpu
from jax.sharding import PartitionSpec as P

HALO = 8
LANES = 128
SHIFTS = 2 * HALO + 1
ALONG = (4, 2, 4, 2)


def exchange_order():
    ys, zs, xs, cores = ALONG
    return [
        ((y * zs + z) * xs + x) * cores + core
        for y in range(ys)
        for x in range(xs)
        for core in range(cores)
        for z in range(zs)
    ]


def pack(coarse_ref, blocks_ref, sems):
    local, _, zs = coarse_ref.shape[:3]
    copies = [
        pltpu.make_async_copy(coarse_ref.at[s, :, z], blocks_ref.at[:, :, z, s], sems.at[s, z])
        for s in range(local)
        for z in range(zs)
    ]
    for copy in copies:
        copy.start()
    for copy in copies:
        copy.wait()


def write_taps(local, offsets_ref, taps_ref):
    spin_count, seg_count = offsets_ref.shape
    ys, zs, xs, cores = ALONG
    source = lax.broadcasted_iota(jnp.int32, (seg_count, seg_count), 0)
    arrival = lax.broadcasted_iota(jnp.int32, (seg_count, seg_count), 1)
    s, device = arrival % local, arrival // local
    z, device = device % zs, device // zs
    core, device = device % cores, device // cores
    x, y = device % xs, device // xs
    natural = (((y * zs + z) * xs + x) * cores + core) * local + s
    move = jnp.where(source == natural, 1.0, 0.0).astype(jnp.bfloat16)
    arrived = jnp.dot(
        offsets_ref[...].astype(jnp.float32).astype(jnp.bfloat16), move, preferred_element_type=jnp.float32
    )
    for index in range(SHIFTS):
        hit = arrived == float(index - HALO)
        taps_ref[pl.ds(index * spin_count, spin_count), :] = jnp.where(hit, 1.0 / seg_count, 0.0).astype(jnp.bfloat16)


def accumulate(local, offsets_ref, maps_ref, fine_ref, msg_ref, rest_ref, data, taps_ref, total, early, late, in_sem, out_sems):
    spin_count, seg_count = offsets_ref.shape
    points = maps_ref.shape[0] // seg_count
    tiles = maps_ref.shape[1] // LANES
    pairs = tiles // 2
    groups = spin_count // 8

    def fetch(tile):
        return pltpu.make_async_copy(
            maps_ref.at[:, pl.ds(tile * LANES, LANES)], data.at[tile], in_sem
        )

    def take(tile):
        for row in range(0, seg_count * points, 8 * points):
            data[tile, pl.ds(row, 8 * points), :] = maps_ref[pl.ds(row, 8 * points), tile * LANES : (tile + 1) * LANES]

    def emit(tile):
        return pltpu.make_async_copy(
            total.at[tile + 1], fine_ref.at[:, pl.ds(tile * LANES, LANES)], out_sems.at[tile]
        )

    take(0)
    take(1)
    write_taps(local, offsets_ref, taps_ref)
    total[...] = jnp.zeros_like(total)
    lane = lax.broadcasted_iota(jnp.int32, (spin_count, LANES), 1)

    def multiply(pair, point, product):
        block = jnp.concatenate(
            [data.at[2 * pair + half][pl.ds(point, seg_count, stride=points), :] for half in range(2)],
            axis=1,
        )
        high = block.astype(jnp.bfloat16)
        low = (block - high.astype(jnp.float32)).astype(jnp.bfloat16)
        taps = taps_ref[...]
        product[...] = jnp.dot(taps, high, preferred_element_type=jnp.float32) + jnp.dot(
            taps, low, preferred_element_type=jnp.float32
        )

    def combine(pair, point, product):
        sums = [jnp.zeros((spin_count, LANES), jnp.float32) for _ in range(4)]
        for index in range(SHIFTS):
            shift = index - HALO
            where = pl.ds(index * spin_count, spin_count)
            left, right = product[where, :LANES], product[where, LANES:]
            if shift == 0:
                sums[1] = sums[1] + left
                sums[2] = sums[2] + right
                continue
            left = pltpu.roll(left, (-shift) % LANES, 1)
            right = pltpu.roll(right, (-shift) % LANES, 1)
            if shift > 0:
                same = lane < LANES - shift
                sums[0] = sums[0] + jnp.where(same, 0.0, left)
                sums[1] = sums[1] + jnp.where(same, left, right)
                sums[2] = sums[2] + jnp.where(same, right, 0.0)
            else:
                same = lane >= -shift
                sums[1] = sums[1] + jnp.where(same, left, 0.0)
                sums[2] = sums[2] + jnp.where(same, right, left)
                sums[3] = sums[3] + jnp.where(same, 0.0, right)
        for place in range(4):
            target = total.at[2 * pair + place]
            for group in range(groups):
                where = pl.ds(group * 8 * points + point, 8, stride=points)
                target[where, :] = target[where, :] + sums[place][group * 8 : group * 8 + 8]

    half = points // 2
    for point in range(half):
        multiply(0, point, early.at[point])
    for tile in range(2, tiles - 1):
        take(tile)
    fetch(tiles - 1).start()
    fetch(tiles - 1).wait()
    for pair in range(pairs):
        for point in range(half):
            multiply(pair, half + point, late.at[point])
            combine(pair, point, early.at[point])
        for point in range(half):
            if pair + 1 < pairs:
                multiply(pair + 1, point, early.at[point])
            combine(pair, half + point, late.at[point])
        if pair + 1 < pairs:
            for tile in range(max(1, 2 * pair - 1), 2 * pair + 1):
                emit(tile).start()

    side = lax.axis_index("freq")
    low_side = side == 0
    row_lane = lax.broadcasted_iota(jnp.int32, (points, LANES), 1)
    outer = row_lane >= LANES - HALO
    inner = row_lane < HALO
    best = jnp.full((points, LANES), -jnp.inf, jnp.float32)
    for spin in range(spin_count):
        where = pl.ds(spin * points, points)
        for tile in range(1, tiles - 1):
            best = jnp.maximum(best, total[tile + 1, where, :])
        first, last = total[1, where, :], total[tiles, where, :]
        best = jnp.maximum(best, jnp.where(row_lane < HALO * side, -jnp.inf, first))
        best = jnp.maximum(best, jnp.where(row_lane >= LANES - HALO * (1 - side), -jnp.inf, last))
    msg_ref[pl.ds(groups * points, points), :] = best
    for group in range(groups):
        packed = jnp.zeros((points, LANES), jnp.float32)
        for slot in range(8):
            where = pl.ds((group * 8 + slot) * points, points)
            first, last = total[1, where, :], total[tiles, where, :]
            before, after = total[0, where, :], total[tiles + 1, where, :]
            mine = jnp.where(
                low_side, jnp.where(inner, after, last), jnp.where(inner, first, before)
            )
            mine = jnp.where(jnp.logical_or(inner, outer), mine, 0.0)
            packed = packed + pltpu.roll(mine, (HALO + 2 * HALO * slot) % LANES, 1)
        msg_ref[pl.ds(group * points, points), :] = packed
    rest_ref[0] = total[1]
    for place in range(3):
        rest_ref[1 + place] = total[tiles - 2 + place]
    for tile in range(1, tiles - 3):
        emit(tile).wait()


def finish(mine_ref, theirs_ref, rest_ref, fine_in, fine_ref, peaks_ref, first, last, sems):
    points = peaks_ref.shape[1]
    groups = mine_ref.shape[0] // points - 1
    tiles = fine_ref.shape[1] // LANES

    def emit(source, tile, place):
        return pltpu.make_async_copy(source, fine_ref.at[:, pl.ds(tile * LANES, LANES)], sems.at[place])

    copies = [
        emit(first, 0, 0),
        emit(rest_ref.at[1], tiles - 3, 1),
        emit(rest_ref.at[2], tiles - 2, 2),
        emit(last, tiles - 1, 3),
    ]
    copies[1].start()
    copies[2].start()
    side = lax.axis_index("freq")
    row_lane = lax.broadcasted_iota(jnp.int32, (points, LANES), 1)
    tail = pl.ds(groups * points, points)
    best = jnp.maximum(mine_ref[tail, :], theirs_ref[tail, :])
    for group in range(groups):
        where = pl.ds(group * points, points)
        packed = mine_ref[where, :] + theirs_ref[where, :]
        best = jnp.maximum(best, packed)
        for slot in range(8):
            rows = pl.ds((group * 8 + slot) * points, points)
            back = pltpu.roll(packed, (-(HALO + 2 * HALO * slot)) % LANES, 1)
            first[rows, :] = jnp.where(row_lane < HALO * side, back, rest_ref[0, rows, :])
            last[rows, :] = jnp.where(row_lane >= LANES - HALO * (1 - side), back, rest_ref[3, rows, :])
    copies[0].start()
    copies[3].start()
    top = jnp.max(best, axis=1, keepdims=True)
    row = lax.broadcasted_iota(jnp.int32, (points, LANES), 0)
    spread = jnp.max(jnp.where(row == row_lane, top, -jnp.inf), axis=0, keepdims=True)
    peaks_ref[...] = spread[:, :points]
    for copy in copies:
        copy.wait()


def on_device(coarse, offsets):
    nseg = lax.axis_size("seg")
    local_segs, points_all, bins = coarse.shape
    points = points_all // nseg
    segs = local_segs * nseg
    spins = offsets.shape[1]
    tiles = bins // LANES
    rows = spins * points
    groups = spins // 8
    ys, zs, xs, cores = ALONG
    vmem = pl.BlockSpec(memory_space=pltpu.VMEM)
    anywhere = pl.BlockSpec(memory_space=pl.ANY)
    mib = 1024 * 1024
    blocks = pl.pallas_call(
        pack,
        out_shape=jax.ShapeDtypeStruct((ys, xs * cores, zs, local_segs, points, bins), jnp.float32),
        in_specs=[anywhere],
        out_specs=vmem,
        scratch_shapes=[pltpu.SemaphoreType.DMA((local_segs, zs))],
        compiler_params=pltpu.CompilerParams(vmem_limit_bytes=44 * mib),
        name="pack",
    )(coarse.reshape(local_segs, ys, zs, xs * cores, points, bins))
    maps = lax.all_to_all(
        blocks.reshape(nseg, local_segs, points, bins),
        "seg",
        split_axis=0,
        concat_axis=0,
        tiled=True,
        axis_index_groups=[exchange_order()],
    )
    fine, mine, rest = pl.pallas_call(
        functools.partial(accumulate, local_segs),
        out_shape=(
            jax.ShapeDtypeStruct((rows, bins), jnp.float32),
            jax.ShapeDtypeStruct(((groups + 1) * points, LANES), jnp.float32),
            jax.ShapeDtypeStruct((4, rows, LANES), jnp.float32),
        ),
        in_specs=[vmem, vmem],
        out_specs=(anywhere, vmem, vmem),
        scratch_shapes=[
            pltpu.VMEM((tiles, segs * points, LANES), jnp.float32),
            pltpu.VMEM((SHIFTS * spins, segs), jnp.bfloat16),
            pltpu.VMEM((tiles + 2, rows, LANES), jnp.float32),
            pltpu.VMEM((points // 2, SHIFTS * spins, 2 * LANES), jnp.float32),
            pltpu.VMEM((points // 2, SHIFTS * spins, 2 * LANES), jnp.float32),
            pltpu.SemaphoreType.DMA,
            pltpu.SemaphoreType.DMA((tiles,)),
        ],
        compiler_params=pltpu.CompilerParams(vmem_limit_bytes=24 * mib),
        name="accumulate",
    )(offsets.T, maps.reshape(segs * points, bins))
    theirs = lax.ppermute(mine, "freq", [(0, 1), (1, 0)])
    fine, peaks = pl.pallas_call(
        finish,
        out_shape=(
            jax.ShapeDtypeStruct((rows, bins), jnp.float32),
            jax.ShapeDtypeStruct((1, points), jnp.float32),
        ),
        in_specs=[vmem, vmem, vmem, anywhere],
        out_specs=(anywhere, vmem),
        scratch_shapes=[
            pltpu.VMEM((rows, LANES), jnp.float32),
            pltpu.VMEM((rows, LANES), jnp.float32),
            pltpu.SemaphoreType.DMA((4,)),
        ],
        input_output_aliases={3: 0},
        compiler_params=pltpu.CompilerParams(vmem_limit_bytes=4 * mib),
        name="finish",
    )(mine, theirs, rest, fine)
    return fine.reshape(spins, points, bins), peaks.reshape(points)


def solution(mesh):
    return jax.shard_map(
        on_device,
        mesh=mesh,
        in_specs=(P("seg", None, "freq"), P()),
        out_specs=(P(None, "seg", "freq"), P("seg")),
        check_vma=False,
    )
```

```python
import functools

import jax
import jax.numpy as jnp
from jax import lax
from jax.experimental import pallas as pl
from jax.experimental.pallas import tpu as pltpu
from jax.sharding import PartitionSpec as P

HALO = 8
LANES = 128
SHIFTS = 2 * HALO + 1
ALONG = (4, 2, 4, 2)


def exchange_order():
    ys, zs, xs, cores = ALONG
    return [
        ((y * zs + z) * xs + x) * cores + core
        for y in range(ys)
        for x in range(xs)
        for core in range(cores)
        for z in range(zs)
    ]


def pack(coarse_ref, blocks_ref, sems):
    local, _, zs = coarse_ref.shape[:3]
    copies = [
        pltpu.make_async_copy(coarse_ref.at[s, :, z], blocks_ref.at[:, :, z, s], sems.at[s, z])
        for s in range(local)
        for z in range(zs)
    ]
    for copy in copies:
        copy.start()
    for copy in copies:
        copy.wait()


def write_taps(local, offsets_ref, taps_ref):
    spin_count, seg_count = offsets_ref.shape
    ys, zs, xs, cores = ALONG
    source = lax.broadcasted_iota(jnp.int32, (seg_count, seg_count), 0)
    arrival = lax.broadcasted_iota(jnp.int32, (seg_count, seg_count), 1)
    s, device = arrival % local, arrival // local
    z, device = device % zs, device // zs
    core, device = device % cores, device // cores
    x, y = device % xs, device // xs
    natural = (((y * zs + z) * xs + x) * cores + core) * local + s
    move = jnp.where(source == natural, 1.0, 0.0).astype(jnp.bfloat16)
    arrived = jnp.dot(
        offsets_ref[...].astype(jnp.float32).astype(jnp.bfloat16), move, preferred_element_type=jnp.float32
    )
    for index in range(SHIFTS):
        hit = arrived == float(index - HALO)
        taps_ref[pl.ds(index * spin_count, spin_count), :] = jnp.where(hit, 1.0 / seg_count, 0.0).astype(jnp.bfloat16)


def accumulate(local, offsets_ref, maps_ref, fine_ref, msg_ref, rest_ref, data, taps_ref, total, early, late, in_sem, out_sems):
    spin_count, seg_count = offsets_ref.shape
    points = maps_ref.shape[0] // seg_count
    tiles = maps_ref.shape[1] // LANES
    pairs = tiles // 2
    groups = spin_count // 8

    def fetch(tile):
        return pltpu.make_async_copy(
            maps_ref.at[:, pl.ds(tile * LANES, LANES)], data.at[tile], in_sem
        )

    def take(tile):
        for row in range(0, seg_count * points, 8 * points):
            data[tile, pl.ds(row, 8 * points), :] = maps_ref[pl.ds(row, 8 * points), tile * LANES : (tile + 1) * LANES]

    def emit(tile):
        return pltpu.make_async_copy(
            total.at[tile + 1], fine_ref.at[:, pl.ds(tile * LANES, LANES)], out_sems.at[tile]
        )

    take(0)
    take(1)
    write_taps(local, offsets_ref, taps_ref)
    total[...] = jnp.zeros_like(total)
    lane = lax.broadcasted_iota(jnp.int32, (8, LANES), 1)

    def multiply(pair, point, product):
        block = jnp.concatenate(
            [data.at[2 * pair + half][pl.ds(point, seg_count, stride=points), :] for half in range(2)],
            axis=1,
        )
        high = block.astype(jnp.bfloat16)
        low = (block - high.astype(jnp.float32)).astype(jnp.bfloat16)
        taps = taps_ref[...]
        product[...] = jnp.dot(taps, high, preferred_element_type=jnp.float32) + jnp.dot(
            taps, low, preferred_element_type=jnp.float32
        )

    def combine(pair, point, product):
        for group in range(groups):
            sums = [jnp.zeros((8, LANES), jnp.float32) for _ in range(4)]
            for index in range(SHIFTS):
                shift = index - HALO
                where = pl.ds(index * spin_count + 8 * group, 8)
                left, right = product[where, :LANES], product[where, LANES:]
                if shift == 0:
                    sums[1] = sums[1] + left
                    sums[2] = sums[2] + right
                    continue
                left = pltpu.roll(left, (-shift) % LANES, 1)
                right = pltpu.roll(right, (-shift) % LANES, 1)
                if shift > 0:
                    same = lane < LANES - shift
                    sums[0] = sums[0] + jnp.where(same, 0.0, left)
                    sums[1] = sums[1] + jnp.where(same, left, right)
                    sums[2] = sums[2] + jnp.where(same, right, 0.0)
                else:
                    same = lane >= -shift
                    sums[1] = sums[1] + jnp.where(same, left, 0.0)
                    sums[2] = sums[2] + jnp.where(same, right, left)
                    sums[3] = sums[3] + jnp.where(same, 0.0, right)
            where = pl.ds(group * 8 * points + point, 8, stride=points)
            for place in range(4):
                target = total.at[2 * pair + place]
                target[where, :] = target[where, :] + sums[place]

    half = points // 2
    for point in range(half):
        multiply(0, point, early.at[point])
    fetch(tiles - 1).start()
    fetch(tiles - 1).wait()
    for pair in range(pairs):
        for tile in range(2 * pair + 2, min(2 * pair + 4, tiles - 1)):
            take(tile)
        for point in range(half):
            multiply(pair, half + point, late.at[point])
            combine(pair, point, early.at[point])
        for point in range(half):
            if pair + 1 < pairs:
                multiply(pair + 1, point, early.at[point])
            combine(pair, half + point, late.at[point])
        if pair + 1 < pairs:
            for tile in range(max(1, 2 * pair - 1), 2 * pair + 1):
                emit(tile).start()

    side = lax.axis_index("freq")
    low_side = side == 0
    row_lane = lax.broadcasted_iota(jnp.int32, (points, LANES), 1)
    outer = row_lane >= LANES - HALO
    inner = row_lane < HALO
    best = jnp.full((points, LANES), -jnp.inf, jnp.float32)
    for spin in range(spin_count):
        where = pl.ds(spin * points, points)
        for tile in range(1, tiles - 1):
            best = jnp.maximum(best, total[tile + 1, where, :])
        first, last = total[1, where, :], total[tiles, where, :]
        best = jnp.maximum(best, jnp.where(row_lane < HALO * side, -jnp.inf, first))
        best = jnp.maximum(best, jnp.where(row_lane >= LANES - HALO * (1 - side), -jnp.inf, last))
    msg_ref[pl.ds(groups * points, points), :] = best
    for group in range(groups):
        packed = jnp.zeros((points, LANES), jnp.float32)
        for slot in range(8):
            where = pl.ds((group * 8 + slot) * points, points)
            first, last = total[1, where, :], total[tiles, where, :]
            before, after = total[0, where, :], total[tiles + 1, where, :]
            mine = jnp.where(
                low_side, jnp.where(inner, after, last), jnp.where(inner, first, before)
            )
            mine = jnp.where(jnp.logical_or(inner, outer), mine, 0.0)
            packed = packed + pltpu.roll(mine, (HALO + 2 * HALO * slot) % LANES, 1)
        msg_ref[pl.ds(group * points, points), :] = packed
    rest_ref[0] = total[1]
    for place in range(3):
        rest_ref[1 + place] = total[tiles - 2 + place]
    for tile in range(1, tiles - 3):
        emit(tile).wait()


def finish(mine_ref, theirs_ref, rest_ref, fine_in, fine_ref, peaks_ref, first, last, sems):
    points = peaks_ref.shape[1]
    groups = mine_ref.shape[0] // points - 1
    tiles = fine_ref.shape[1] // LANES

    def emit(source, tile, place):
        return pltpu.make_async_copy(source, fine_ref.at[:, pl.ds(tile * LANES, LANES)], sems.at[place])

    copies = [
        emit(first, 0, 0),
        emit(rest_ref.at[1], tiles - 3, 1),
        emit(rest_ref.at[2], tiles - 2, 2),
        emit(last, tiles - 1, 3),
    ]
    copies[1].start()
    copies[2].start()
    side = lax.axis_index("freq")
    row_lane = lax.broadcasted_iota(jnp.int32, (points, LANES), 1)
    tail = pl.ds(groups * points, points)
    best = jnp.maximum(mine_ref[tail, :], theirs_ref[tail, :])
    for group in range(groups):
        where = pl.ds(group * points, points)
        packed = mine_ref[where, :] + theirs_ref[where, :]
        best = jnp.maximum(best, packed)
        for slot in range(8):
            rows = pl.ds((group * 8 + slot) * points, points)
            back = pltpu.roll(packed, (-(HALO + 2 * HALO * slot)) % LANES, 1)
            first[rows, :] = jnp.where(row_lane < HALO * side, back, rest_ref[0, rows, :])
            last[rows, :] = jnp.where(row_lane >= LANES - HALO * (1 - side), back, rest_ref[3, rows, :])
    copies[0].start()
    copies[3].start()
    top = jnp.max(best, axis=1, keepdims=True)
    row = lax.broadcasted_iota(jnp.int32, (points, LANES), 0)
    spread = jnp.max(jnp.where(row == row_lane, top, -jnp.inf), axis=0, keepdims=True)
    peaks_ref[...] = spread[:, :points]
    for copy in copies:
        copy.wait()


def on_device(coarse, offsets):
    nseg = lax.axis_size("seg")
    local_segs, points_all, bins = coarse.shape
    points = points_all // nseg
    segs = local_segs * nseg
    spins = offsets.shape[1]
    tiles = bins // LANES
    rows = spins * points
    groups = spins // 8
    ys, zs, xs, cores = ALONG
    vmem = pl.BlockSpec(memory_space=pltpu.VMEM)
    anywhere = pl.BlockSpec(memory_space=pl.ANY)
    mib = 1024 * 1024
    blocks = pl.pallas_call(
        pack,
        out_shape=jax.ShapeDtypeStruct((ys, xs * cores, zs, local_segs, points, bins), jnp.float32),
        in_specs=[anywhere],
        out_specs=vmem,
        scratch_shapes=[pltpu.SemaphoreType.DMA((local_segs, zs))],
        compiler_params=pltpu.CompilerParams(vmem_limit_bytes=44 * mib),
        name="pack",
    )(coarse.reshape(local_segs, ys, zs, xs * cores, points, bins))
    maps = lax.all_to_all(
        blocks.reshape(nseg, local_segs, points, bins),
        "seg",
        split_axis=0,
        concat_axis=0,
        tiled=True,
        axis_index_groups=[exchange_order()],
    )
    fine, mine, rest = pl.pallas_call(
        functools.partial(accumulate, local_segs),
        out_shape=(
            jax.ShapeDtypeStruct((rows, bins), jnp.float32),
            jax.ShapeDtypeStruct(((groups + 1) * points, LANES), jnp.float32),
            jax.ShapeDtypeStruct((4, rows, LANES), jnp.float32),
        ),
        in_specs=[vmem, vmem],
        out_specs=(anywhere, vmem, vmem),
        scratch_shapes=[
            pltpu.VMEM((tiles, segs * points, LANES), jnp.float32),
            pltpu.VMEM((SHIFTS * spins, segs), jnp.bfloat16),
            pltpu.VMEM((tiles + 2, rows, LANES), jnp.float32),
            pltpu.VMEM((points // 2, SHIFTS * spins, 2 * LANES), jnp.float32),
            pltpu.VMEM((points // 2, SHIFTS * spins, 2 * LANES), jnp.float32),
            pltpu.SemaphoreType.DMA,
            pltpu.SemaphoreType.DMA((tiles,)),
        ],
        compiler_params=pltpu.CompilerParams(vmem_limit_bytes=24 * mib),
        name="accumulate",
    )(offsets.T, maps.reshape(segs * points, bins))
    theirs = lax.ppermute(mine, "freq", [(0, 1), (1, 0)])
    fine, peaks = pl.pallas_call(
        finish,
        out_shape=(
            jax.ShapeDtypeStruct((rows, bins), jnp.float32),
            jax.ShapeDtypeStruct((1, points), jnp.float32),
        ),
        in_specs=[vmem, vmem, vmem, anywhere],
        out_specs=(anywhere, vmem),
        scratch_shapes=[
            pltpu.VMEM((rows, LANES), jnp.float32),
            pltpu.VMEM((rows, LANES), jnp.float32),
            pltpu.SemaphoreType.DMA((4,)),
        ],
        input_output_aliases={3: 0},
        compiler_params=pltpu.CompilerParams(vmem_limit_bytes=4 * mib),
        name="finish",
    )(mine, theirs, rest, fine)
    return fine.reshape(spins, points, bins), peaks.reshape(points)


def solution(mesh):
    return jax.shard_map(
        on_device,
        mesh=mesh,
        in_specs=(P("seg", None, "freq"), P()),
        out_specs=(P(None, "seg", "freq"), P("seg")),
        check_vma=False,
    )
```

```python
import functools

import jax
import jax.numpy as jnp
from jax import lax
from jax.experimental import pallas as pl
from jax.experimental.pallas import tpu as pltpu
from jax.sharding import PartitionSpec as P

HALO = 8
LANES = 128
SHIFTS = 2 * HALO + 1
ALONG = (4, 2, 4, 2)


def exchange_order():
    ys, zs, xs, cores = ALONG
    return [
        ((y * zs + z) * xs + x) * cores + core
        for y in range(ys)
        for x in range(xs)
        for z in range(zs)
        for core in range(cores)
    ]


def pack(coarse_ref, blocks_ref, sems):
    local, _, zs = coarse_ref.shape[:3]
    copies = [
        pltpu.make_async_copy(coarse_ref.at[s, :, z], blocks_ref.at[:, :, z, :, s], sems.at[s, z])
        for s in range(local)
        for z in range(zs)
    ]
    for copy in copies:
        copy.start()
    for copy in copies:
        copy.wait()


def write_taps(local, offsets_ref, taps_ref):
    spin_count, seg_count = offsets_ref.shape
    ys, zs, xs, cores = ALONG
    source = lax.broadcasted_iota(jnp.int32, (seg_count, seg_count), 0)
    arrival = lax.broadcasted_iota(jnp.int32, (seg_count, seg_count), 1)
    s, device = arrival % local, arrival // local
    core, device = device % cores, device // cores
    z, device = device % zs, device // zs
    x, y = device % xs, device // xs
    natural = (((y * zs + z) * xs + x) * cores + core) * local + s
    move = jnp.where(source == natural, 1.0, 0.0).astype(jnp.bfloat16)
    arrived = jnp.dot(
        offsets_ref[...].astype(jnp.float32).astype(jnp.bfloat16), move, preferred_element_type=jnp.float32
    )
    for index in range(SHIFTS):
        hit = arrived == float(index - HALO)
        taps_ref[pl.ds(index * spin_count, spin_count), :] = jnp.where(hit, 1.0 / seg_count, 0.0).astype(jnp.bfloat16)


def accumulate(local, offsets_ref, maps_ref, fine_ref, msg_ref, rest_ref, data, taps_ref, total, early, late, in_sem, out_sems):
    spin_count, seg_count = offsets_ref.shape
    points = maps_ref.shape[0] // seg_count
    tiles = maps_ref.shape[1] // LANES
    pairs = tiles // 2
    groups = spin_count // 8

    def fetch(tile):
        return pltpu.make_async_copy(
            maps_ref.at[:, pl.ds(tile * LANES, LANES)], data.at[tile], in_sem
        )

    def take(tile):
        for row in range(0, seg_count * points, 8 * points):
            data[tile, pl.ds(row, 8 * points), :] = maps_ref[pl.ds(row, 8 * points), tile * LANES : (tile + 1) * LANES]

    def emit(tile):
        return pltpu.make_async_copy(
            total.at[tile + 1], fine_ref.at[:, pl.ds(tile * LANES, LANES)], out_sems.at[tile]
        )

    take(0)
    take(1)
    write_taps(local, offsets_ref, taps_ref)
    total[...] = jnp.zeros_like(total)
    lane = lax.broadcasted_iota(jnp.int32, (8, LANES), 1)

    def multiply(pair, point, product):
        block = jnp.concatenate(
            [data.at[2 * pair + half][pl.ds(point, seg_count, stride=points), :] for half in range(2)],
            axis=1,
        )
        high = block.astype(jnp.bfloat16)
        low = (block - high.astype(jnp.float32)).astype(jnp.bfloat16)
        taps = taps_ref[...]
        product[...] = jnp.dot(taps, high, preferred_element_type=jnp.float32) + jnp.dot(
            taps, low, preferred_element_type=jnp.float32
        )

    def combine(pair, point, product):
        for group in range(groups):
            sums = [jnp.zeros((8, LANES), jnp.float32) for _ in range(4)]
            for index in range(SHIFTS):
                shift = index - HALO
                where = pl.ds(index * spin_count + 8 * group, 8)
                left, right = product[where, :LANES], product[where, LANES:]
                if shift == 0:
                    sums[1] = sums[1] + left
                    sums[2] = sums[2] + right
                    continue
                left = pltpu.roll(left, (-shift) % LANES, 1)
                right = pltpu.roll(right, (-shift) % LANES, 1)
                if shift > 0:
                    same = lane < LANES - shift
                    sums[0] = sums[0] + jnp.where(same, 0.0, left)
                    sums[1] = sums[1] + jnp.where(same, left, right)
                    sums[2] = sums[2] + jnp.where(same, right, 0.0)
                else:
                    same = lane >= -shift
                    sums[1] = sums[1] + jnp.where(same, left, 0.0)
                    sums[2] = sums[2] + jnp.where(same, right, left)
                    sums[3] = sums[3] + jnp.where(same, 0.0, right)
            where = pl.ds(group * 8 * points + point, 8, stride=points)
            for place in range(4):
                target = total.at[2 * pair + place]
                target[where, :] = target[where, :] + sums[place]

    half = points // 2
    for point in range(half):
        multiply(0, point, early.at[point])
    fetch(tiles - 1).start()
    fetch(tiles - 1).wait()
    for pair in range(pairs):
        for tile in range(2 * pair + 2, min(2 * pair + 4, tiles - 1)):
            take(tile)
        for point in range(half):
            multiply(pair, half + point, late.at[point])
            combine(pair, point, early.at[point])
        for point in range(half):
            if pair + 1 < pairs:
                multiply(pair + 1, point, early.at[point])
            combine(pair, half + point, late.at[point])
        if pair + 1 < pairs:
            for tile in range(max(1, 2 * pair - 1), 2 * pair + 1):
                emit(tile).start()

    side = lax.axis_index("freq")
    low_side = side == 0
    row_lane = lax.broadcasted_iota(jnp.int32, (points, LANES), 1)
    outer = row_lane >= LANES - HALO
    inner = row_lane < HALO
    best = jnp.full((points, LANES), -jnp.inf, jnp.float32)
    for spin in range(spin_count):
        where = pl.ds(spin * points, points)
        for tile in range(1, tiles - 1):
            best = jnp.maximum(best, total[tile + 1, where, :])
        first, last = total[1, where, :], total[tiles, where, :]
        best = jnp.maximum(best, jnp.where(row_lane < HALO * side, -jnp.inf, first))
        best = jnp.maximum(best, jnp.where(row_lane >= LANES - HALO * (1 - side), -jnp.inf, last))
    msg_ref[pl.ds(groups * points, points), :] = best
    for group in range(groups):
        packed = jnp.zeros((points, LANES), jnp.float32)
        for slot in range(8):
            where = pl.ds((group * 8 + slot) * points, points)
            first, last = total[1, where, :], total[tiles, where, :]
            before, after = total[0, where, :], total[tiles + 1, where, :]
            mine = jnp.where(
                low_side, jnp.where(inner, after, last), jnp.where(inner, first, before)
            )
            mine = jnp.where(jnp.logical_or(inner, outer), mine, 0.0)
            packed = packed + pltpu.roll(mine, (HALO + 2 * HALO * slot) % LANES, 1)
        msg_ref[pl.ds(group * points, points), :] = packed
    rest_ref[0] = total[1]
    for place in range(3):
        rest_ref[1 + place] = total[tiles - 2 + place]
    for tile in range(1, tiles - 3):
        emit(tile).wait()


def finish(mine_ref, theirs_ref, rest_ref, fine_in, fine_ref, peaks_ref, first, last, sems):
    points = peaks_ref.shape[1]
    groups = mine_ref.shape[0] // points - 1
    tiles = fine_ref.shape[1] // LANES

    def emit(source, tile, place):
        return pltpu.make_async_copy(source, fine_ref.at[:, pl.ds(tile * LANES, LANES)], sems.at[place])

    copies = [
        emit(first, 0, 0),
        emit(rest_ref.at[1], tiles - 3, 1),
        emit(rest_ref.at[2], tiles - 2, 2),
        emit(last, tiles - 1, 3),
    ]
    copies[1].start()
    copies[2].start()
    side = lax.axis_index("freq")
    row_lane = lax.broadcasted_iota(jnp.int32, (points, LANES), 1)
    tail = pl.ds(groups * points, points)
    best = jnp.maximum(mine_ref[tail, :], theirs_ref[tail, :])
    for group in range(groups):
        where = pl.ds(group * points, points)
        packed = mine_ref[where, :] + theirs_ref[where, :]
        best = jnp.maximum(best, packed)
        for slot in range(8):
            rows = pl.ds((group * 8 + slot) * points, points)
            back = pltpu.roll(packed, (-(HALO + 2 * HALO * slot)) % LANES, 1)
            first[rows, :] = jnp.where(row_lane < HALO * side, back, rest_ref[0, rows, :])
            last[rows, :] = jnp.where(row_lane >= LANES - HALO * (1 - side), back, rest_ref[3, rows, :])
    copies[0].start()
    copies[3].start()
    top = jnp.max(best, axis=1, keepdims=True)
    row = lax.broadcasted_iota(jnp.int32, (points, LANES), 0)
    spread = jnp.max(jnp.where(row == row_lane, top, -jnp.inf), axis=0, keepdims=True)
    peaks_ref[...] = spread[:, :points]
    for copy in copies:
        copy.wait()


def on_device(coarse, offsets):
    nseg = lax.axis_size("seg")
    local_segs, points_all, bins = coarse.shape
    points = points_all // nseg
    segs = local_segs * nseg
    spins = offsets.shape[1]
    tiles = bins // LANES
    rows = spins * points
    groups = spins // 8
    ys, zs, xs, cores = ALONG
    vmem = pl.BlockSpec(memory_space=pltpu.VMEM)
    anywhere = pl.BlockSpec(memory_space=pl.ANY)
    mib = 1024 * 1024
    blocks = pl.pallas_call(
        pack,
        out_shape=jax.ShapeDtypeStruct((ys, xs, zs, cores, local_segs, points, bins), jnp.float32),
        in_specs=[anywhere],
        out_specs=vmem,
        scratch_shapes=[pltpu.SemaphoreType.DMA((local_segs, zs))],
        compiler_params=pltpu.CompilerParams(vmem_limit_bytes=44 * mib),
        name="pack",
    )(coarse.reshape(local_segs, ys, zs, xs, cores, points, bins))
    maps = lax.all_to_all(
        blocks.reshape(nseg, local_segs, points, bins),
        "seg",
        split_axis=0,
        concat_axis=0,
        tiled=True,
        axis_index_groups=[exchange_order()],
    )
    fine, mine, rest = pl.pallas_call(
        functools.partial(accumulate, local_segs),
        out_shape=(
            jax.ShapeDtypeStruct((rows, bins), jnp.float32),
            jax.ShapeDtypeStruct(((groups + 1) * points, LANES), jnp.float32),
            jax.ShapeDtypeStruct((4, rows, LANES), jnp.float32),
        ),
        in_specs=[vmem, vmem],
        out_specs=(anywhere, vmem, vmem),
        scratch_shapes=[
            pltpu.VMEM((tiles, segs * points, LANES), jnp.float32),
            pltpu.VMEM((SHIFTS * spins, segs), jnp.bfloat16),
            pltpu.VMEM((tiles + 2, rows, LANES), jnp.float32),
            pltpu.VMEM((points // 2, SHIFTS * spins, 2 * LANES), jnp.float32),
            pltpu.VMEM((points // 2, SHIFTS * spins, 2 * LANES), jnp.float32),
            pltpu.SemaphoreType.DMA,
            pltpu.SemaphoreType.DMA((tiles,)),
        ],
        compiler_params=pltpu.CompilerParams(vmem_limit_bytes=24 * mib),
        name="accumulate",
    )(offsets.T, maps.reshape(segs * points, bins))
    theirs = lax.ppermute(mine, "freq", [(0, 1), (1, 0)])
    fine, peaks = pl.pallas_call(
        finish,
        out_shape=(
            jax.ShapeDtypeStruct((rows, bins), jnp.float32),
            jax.ShapeDtypeStruct((1, points), jnp.float32),
        ),
        in_specs=[vmem, vmem, vmem, anywhere],
        out_specs=(anywhere, vmem),
        scratch_shapes=[
            pltpu.VMEM((rows, LANES), jnp.float32),
            pltpu.VMEM((rows, LANES), jnp.float32),
            pltpu.SemaphoreType.DMA((4,)),
        ],
        input_output_aliases={3: 0},
        compiler_params=pltpu.CompilerParams(vmem_limit_bytes=4 * mib),
        name="finish",
    )(mine, theirs, rest, fine)
    return fine.reshape(spins, points, bins), peaks.reshape(points)


def solution(mesh):
    return jax.shard_map(
        on_device,
        mesh=mesh,
        in_specs=(P("seg", None, "freq"), P()),
        out_specs=(P(None, "seg", "freq"), P("seg")),
        check_vma=False,
    )
```

```python
import functools

import jax
import jax.numpy as jnp
from jax import lax
from jax.experimental import pallas as pl
from jax.experimental.pallas import tpu as pltpu
from jax.sharding import PartitionSpec as P

HALO = 8
LANES = 128
SHIFTS = 2 * HALO + 1
ALONG = (4, 2, 4, 2)


def exchange_order():
    ys, zs, xs, cores = ALONG
    return [
        ((y * zs + z) * xs + x) * cores + core
        for y in range(ys)
        for core in range(cores)
        for x in range(xs)
        for z in range(zs)
    ]


def pack(coarse_ref, blocks_ref, sems):
    local, _, zs, _, cores = coarse_ref.shape[:5]
    copies = [
        pltpu.make_async_copy(
            coarse_ref.at[s, :, z, :, core], blocks_ref.at[:, core, :, z, s], sems.at[s, z, core]
        )
        for s in range(local)
        for z in range(zs)
        for core in range(cores)
    ]
    for copy in copies:
        copy.start()
    for copy in copies:
        copy.wait()


def write_taps(local, offsets_ref, taps_ref):
    spin_count, seg_count = offsets_ref.shape
    ys, zs, xs, cores = ALONG
    source = lax.broadcasted_iota(jnp.int32, (seg_count, seg_count), 0)
    arrival = lax.broadcasted_iota(jnp.int32, (seg_count, seg_count), 1)
    s, device = arrival % local, arrival // local
    z, device = device % zs, device // zs
    x, device = device % xs, device // xs
    core, y = device % cores, device // cores
    natural = (((y * zs + z) * xs + x) * cores + core) * local + s
    move = jnp.where(source == natural, 1.0, 0.0).astype(jnp.bfloat16)
    arrived = jnp.dot(
        offsets_ref[...].astype(jnp.float32).astype(jnp.bfloat16), move, preferred_element_type=jnp.float32
    )
    for index in range(SHIFTS):
        hit = arrived == float(index - HALO)
        taps_ref[pl.ds(index * spin_count, spin_count), :] = jnp.where(hit, 1.0 / seg_count, 0.0).astype(jnp.bfloat16)


def accumulate(local, offsets_ref, maps_ref, fine_ref, msg_ref, rest_ref, data, taps_ref, total, early, late, in_sem, out_sems):
    spin_count, seg_count = offsets_ref.shape
    points = maps_ref.shape[0] // seg_count
    tiles = maps_ref.shape[1] // LANES
    pairs = tiles // 2
    groups = spin_count // 8

    def fetch(tile):
        return pltpu.make_async_copy(
            maps_ref.at[:, pl.ds(tile * LANES, LANES)], data.at[tile], in_sem
        )

    def take(tile):
        for row in range(0, seg_count * points, 8 * points):
            data[tile, pl.ds(row, 8 * points), :] = maps_ref[pl.ds(row, 8 * points), tile * LANES : (tile + 1) * LANES]

    def emit(tile):
        return pltpu.make_async_copy(
            total.at[tile + 1], fine_ref.at[:, pl.ds(tile * LANES, LANES)], out_sems.at[tile]
        )

    take(0)
    take(1)
    write_taps(local, offsets_ref, taps_ref)
    total[...] = jnp.zeros_like(total)
    lane = lax.broadcasted_iota(jnp.int32, (8, LANES), 1)

    def multiply(pair, point, product):
        block = jnp.concatenate(
            [data.at[2 * pair + half][pl.ds(point, seg_count, stride=points), :] for half in range(2)],
            axis=1,
        )
        high = block.astype(jnp.bfloat16)
        low = (block - high.astype(jnp.float32)).astype(jnp.bfloat16)
        taps = taps_ref[...]
        product[...] = jnp.dot(taps, high, preferred_element_type=jnp.float32) + jnp.dot(
            taps, low, preferred_element_type=jnp.float32
        )

    def combine(pair, point, product):
        for group in range(groups):
            sums = [jnp.zeros((8, LANES), jnp.float32) for _ in range(4)]
            for index in range(SHIFTS):
                shift = index - HALO
                where = pl.ds(index * spin_count + 8 * group, 8)
                left, right = product[where, :LANES], product[where, LANES:]
                if shift == 0:
                    sums[1] = sums[1] + left
                    sums[2] = sums[2] + right
                    continue
                left = pltpu.roll(left, (-shift) % LANES, 1)
                right = pltpu.roll(right, (-shift) % LANES, 1)
                if shift > 0:
                    same = lane < LANES - shift
                    sums[0] = sums[0] + jnp.where(same, 0.0, left)
                    sums[1] = sums[1] + jnp.where(same, left, right)
                    sums[2] = sums[2] + jnp.where(same, right, 0.0)
                else:
                    same = lane >= -shift
                    sums[1] = sums[1] + jnp.where(same, left, 0.0)
                    sums[2] = sums[2] + jnp.where(same, right, left)
                    sums[3] = sums[3] + jnp.where(same, 0.0, right)
            where = pl.ds(group * 8 * points + point, 8, stride=points)
            for place in range(4):
                target = total.at[2 * pair + place]
                target[where, :] = target[where, :] + sums[place]

    half = points // 2
    for point in range(half):
        multiply(0, point, early.at[point])
    fetch(tiles - 1).start()
    fetch(tiles - 1).wait()
    for pair in range(pairs):
        for tile in range(2 * pair + 2, min(2 * pair + 4, tiles - 1)):
            take(tile)
        for point in range(half):
            multiply(pair, half + point, late.at[point])
            combine(pair, point, early.at[point])
        for point in range(half):
            if pair + 1 < pairs:
                multiply(pair + 1, point, early.at[point])
            combine(pair, half + point, late.at[point])
        if pair + 1 < pairs:
            for tile in range(max(1, 2 * pair - 1), 2 * pair + 1):
                emit(tile).start()

    side = lax.axis_index("freq")
    low_side = side == 0
    row_lane = lax.broadcasted_iota(jnp.int32, (points, LANES), 1)
    outer = row_lane >= LANES - HALO
    inner = row_lane < HALO
    best = jnp.full((points, LANES), -jnp.inf, jnp.float32)
    for spin in range(spin_count):
        where = pl.ds(spin * points, points)
        for tile in range(1, tiles - 1):
            best = jnp.maximum(best, total[tile + 1, where, :])
        first, last = total[1, where, :], total[tiles, where, :]
        best = jnp.maximum(best, jnp.where(row_lane < HALO * side, -jnp.inf, first))
        best = jnp.maximum(best, jnp.where(row_lane >= LANES - HALO * (1 - side), -jnp.inf, last))
    msg_ref[pl.ds(groups * points, points), :] = best
    for group in range(groups):
        packed = jnp.zeros((points, LANES), jnp.float32)
        for slot in range(8):
            where = pl.ds((group * 8 + slot) * points, points)
            first, last = total[1, where, :], total[tiles, where, :]
            before, after = total[0, where, :], total[tiles + 1, where, :]
            mine = jnp.where(
                low_side, jnp.where(inner, after, last), jnp.where(inner, first, before)
            )
            mine = jnp.where(jnp.logical_or(inner, outer), mine, 0.0)
            packed = packed + pltpu.roll(mine, (HALO + 2 * HALO * slot) % LANES, 1)
        msg_ref[pl.ds(group * points, points), :] = packed
    rest_ref[0] = total[1]
    for place in range(3):
        rest_ref[1 + place] = total[tiles - 2 + place]
    for tile in range(1, tiles - 3):
        emit(tile).wait()


def finish(mine_ref, theirs_ref, rest_ref, fine_in, fine_ref, peaks_ref, first, last, sems):
    points = peaks_ref.shape[1]
    groups = mine_ref.shape[0] // points - 1
    tiles = fine_ref.shape[1] // LANES

    def emit(source, tile, place):
        return pltpu.make_async_copy(source, fine_ref.at[:, pl.ds(tile * LANES, LANES)], sems.at[place])

    copies = [
        emit(first, 0, 0),
        emit(rest_ref.at[1], tiles - 3, 1),
        emit(rest_ref.at[2], tiles - 2, 2),
        emit(last, tiles - 1, 3),
    ]
    copies[1].start()
    copies[2].start()
    side = lax.axis_index("freq")
    row_lane = lax.broadcasted_iota(jnp.int32, (points, LANES), 1)
    tail = pl.ds(groups * points, points)
    best = jnp.maximum(mine_ref[tail, :], theirs_ref[tail, :])
    for group in range(groups):
        where = pl.ds(group * points, points)
        packed = mine_ref[where, :] + theirs_ref[where, :]
        best = jnp.maximum(best, packed)
        for slot in range(8):
            rows = pl.ds((group * 8 + slot) * points, points)
            back = pltpu.roll(packed, (-(HALO + 2 * HALO * slot)) % LANES, 1)
            first[rows, :] = jnp.where(row_lane < HALO * side, back, rest_ref[0, rows, :])
            last[rows, :] = jnp.where(row_lane >= LANES - HALO * (1 - side), back, rest_ref[3, rows, :])
    copies[0].start()
    copies[3].start()
    top = jnp.max(best, axis=1, keepdims=True)
    row = lax.broadcasted_iota(jnp.int32, (points, LANES), 0)
    spread = jnp.max(jnp.where(row == row_lane, top, -jnp.inf), axis=0, keepdims=True)
    peaks_ref[...] = spread[:, :points]
    for copy in copies:
        copy.wait()


def on_device(coarse, offsets):
    nseg = lax.axis_size("seg")
    local_segs, points_all, bins = coarse.shape
    points = points_all // nseg
    segs = local_segs * nseg
    spins = offsets.shape[1]
    tiles = bins // LANES
    rows = spins * points
    groups = spins // 8
    ys, zs, xs, cores = ALONG
    vmem = pl.BlockSpec(memory_space=pltpu.VMEM)
    anywhere = pl.BlockSpec(memory_space=pl.ANY)
    mib = 1024 * 1024
    blocks = pl.pallas_call(
        pack,
        out_shape=jax.ShapeDtypeStruct((ys, cores, xs, zs, local_segs, points, bins), jnp.float32),
        in_specs=[anywhere],
        out_specs=vmem,
        scratch_shapes=[pltpu.SemaphoreType.DMA((local_segs, zs, cores))],
        compiler_params=pltpu.CompilerParams(vmem_limit_bytes=44 * mib),
        name="pack",
    )(coarse.reshape(local_segs, ys, zs, xs, cores, points, bins))
    maps = lax.all_to_all(
        blocks.reshape(nseg, local_segs, points, bins),
        "seg",
        split_axis=0,
        concat_axis=0,
        tiled=True,
        axis_index_groups=[exchange_order()],
    )
    fine, mine, rest = pl.pallas_call(
        functools.partial(accumulate, local_segs),
        out_shape=(
            jax.ShapeDtypeStruct((rows, bins), jnp.float32),
            jax.ShapeDtypeStruct(((groups + 1) * points, LANES), jnp.float32),
            jax.ShapeDtypeStruct((4, rows, LANES), jnp.float32),
        ),
        in_specs=[vmem, vmem],
        out_specs=(anywhere, vmem, vmem),
        scratch_shapes=[
            pltpu.VMEM((tiles, segs * points, LANES), jnp.float32),
            pltpu.VMEM((SHIFTS * spins, segs), jnp.bfloat16),
            pltpu.VMEM((tiles + 2, rows, LANES), jnp.float32),
            pltpu.VMEM((points // 2, SHIFTS * spins, 2 * LANES), jnp.float32),
            pltpu.VMEM((points // 2, SHIFTS * spins, 2 * LANES), jnp.float32),
            pltpu.SemaphoreType.DMA,
            pltpu.SemaphoreType.DMA((tiles,)),
        ],
        compiler_params=pltpu.CompilerParams(vmem_limit_bytes=24 * mib),
        name="accumulate",
    )(offsets.T, maps.reshape(segs * points, bins))
    theirs = lax.ppermute(mine, "freq", [(0, 1), (1, 0)])
    fine, peaks = pl.pallas_call(
        finish,
        out_shape=(
            jax.ShapeDtypeStruct((rows, bins), jnp.float32),
            jax.ShapeDtypeStruct((1, points), jnp.float32),
        ),
        in_specs=[vmem, vmem, vmem, anywhere],
        out_specs=(anywhere, vmem),
        scratch_shapes=[
            pltpu.VMEM((rows, LANES), jnp.float32),
            pltpu.VMEM((rows, LANES), jnp.float32),
            pltpu.SemaphoreType.DMA((4,)),
        ],
        input_output_aliases={3: 0},
        compiler_params=pltpu.CompilerParams(vmem_limit_bytes=4 * mib),
        name="finish",
    )(mine, theirs, rest, fine)
    return fine.reshape(spins, points, bins), peaks.reshape(points)


def solution(mesh):
    return jax.shard_map(
        on_device,
        mesh=mesh,
        in_specs=(P("seg", None, "freq"), P()),
        out_specs=(P(None, "seg", "freq"), P("seg")),
        check_vma=False,
    )
```
